128 devices in a mesh: inst: 2 (over core), pipe: 8 (over x_lo, z), tensor: 8 (over x_hi, y).
Axes of the slice: x: 4 (x_hi: 2, x_lo: 2; x = x_hi * 2 + x_lo), y: 4, z: 4, core: 2. Of those that a mesh axis runs over, the one named last changes fastest.
Arguments:
- lengths: int32 [2, 64], replicated, may hold values from 2 to 384, as said below
- page_table: int32 [2, 64, 3], P('inst'), may hold values from 0 to 191, as said below
- migration: int32 [16, 3], replicated, may hold values from 0 to 63, as said below
- dest_slots: int32 [16, 3], replicated, may hold values from 0 to 47, as said below
- queries: bfloat16 [2, 8, 64, 8192], P('inst', 'pipe', None, 'tensor'), may hold values from -64 to 64
- key_cache: bfloat16 [2, 8, 8, 24576, 128], P('inst', 'pipe', 'tensor'), may hold values from -64 to 64
- value_cache: bfloat16 [2, 8, 8, 24576, 128], P('inst', 'pipe', 'tensor'), may hold values from -5 to 5
- out_weight: bfloat16 [8, 8192, 8192], P('pipe', 'tensor'), may hold values from -0.09375 to 0.09375
Outputs:
- update: bfloat16 [2, 64, 8192], P('inst', None, ('pipe', 'tensor'))
- received_keys: bfloat16 [2, 8, 8, 6144, 128], P('inst', 'pipe', 'tensor')
- received_values: bfloat16 [2, 8, 8, 6144, 128], P('inst', 'pipe', 'tensor')
The draws below stay inside these ranges and needn't reach their ends.
Inputs may be any that keep to these rules, and one draw needn't show every extreme that they name: `lengths`: in instance 1 every request holds more than 192 tokens and one holds exactly 384; in instance 0 every request holds at most 192. `page_table`: for each instance a permutation of its 192 pool pages, 3 for each request. `migration`: rows 0 to 7 name source instance 1 and destination instance 0, the other rows source 0 and destination 1; the requests of all rows are distinct numbers, and the one in row 0 holds at most (2) * 128 tokens. `dest_slots`: A permutation of the 48 receive slots.
All inputs are finite; a program needn't handle non-finite values.
Results may differ from the reference program's by a relative error of at most 0.018.
Values may be sent and summed in bfloat16 or wider, within the bound.
No kernel may reach another device: no remote copies, remote signals or barrier semaphores. Data moves between devices by JAX's collectives and lax.ppermute only.
A program may use at most 128 MiB of HBM per device.

```python
import math
import jax
import jax.numpy as jnp
from jax import lax

D = 8192
HEADS = 64
KVH = 8
HD = 128
PAGE = 128
MAXP = 3
ROWS = 64
LAYERS = 8
MOVE = 16
POOL = 192
RECV = 48
N_INST = 2


def layout(key):
    base_key = jax.random.fold_in(key, 11)
    subkeys = jax.random.split(base_key, 7)
    full_length = MAXP * PAGE
    half_length = full_length // 2
    heavy_side = 1
    half_move = MOVE // 2
    order = jax.random.permutation(subkeys[4], ROWS)
    chosen = order[:MOVE]
    longest_row = order[ROWS - 1]
    long_lengths = jax.random.randint(subkeys[1], (ROWS,), half_length + 1, full_length + 1)
    first_length = jax.random.randint(subkeys[2], (), half_length + 1, (MAXP - 1) * PAGE + 1)
    long_lengths = jnp.where(jnp.arange(ROWS) == chosen[0], first_length, long_lengths)
    long_lengths = jnp.where(jnp.arange(ROWS) == longest_row, full_length, long_lengths)
    short_lengths = jax.random.randint(subkeys[3], (ROWS,), 2, half_length + 1)
    is_heavy = (jnp.arange(N_INST) == heavy_side)[:, None]
    lengths = jnp.where(is_heavy, long_lengths[None, :], short_lengths[None, :]).astype(jnp.int32)
    from_heavy = jnp.arange(MOVE) < half_move
    source_col = jnp.where(from_heavy, heavy_side, 1 - heavy_side)
    target_col = 1 - source_col
    migration = jnp.stack([chosen, source_col, target_col], axis=1).astype(jnp.int32)
    table_keys = jax.random.split(subkeys[5], N_INST)
    page_table = jnp.stack([jax.random.permutation(table_keys[index], POOL) for index in range(N_INST)]).reshape(N_INST, ROWS, MAXP).astype(jnp.int32)
    dest_slots = jax.random.permutation(subkeys[6], RECV).reshape(MOVE, MAXP).astype(jnp.int32)
    return (lengths, page_table, migration, dest_slots)


def draw_lengths(key, part):
    return layout(key)[0]


def draw_page_table(key, part):
    return layout(key)[1]


def draw_migration(key, part):
    return layout(key)[2]


def draw_dest_slots(key, part):
    return layout(key)[3]


def draw_queries(key, part):
    drawn = jnp.clip(jax.random.normal(jax.random.fold_in(key, 41), (N_INST, LAYERS, ROWS, HEADS * HD), jnp.float32), -4.0, 4.0)
    return drawn.astype(jnp.bfloat16)


def draw_key_cache(key, part):
    drawn = jnp.clip(jax.random.normal(jax.random.fold_in(key, 21), (N_INST, LAYERS, KVH, POOL * PAGE, HD), jnp.float32), -4.0, 4.0)
    return drawn.astype(jnp.bfloat16)


def raised(entries, key, source, target, blocks, factor):
    owner, partner = [(jnp.arange(entries.shape[axis_at]) // (entries.shape[axis_at] // blocks)).reshape([-1 if axis == axis_at else 1 for axis in range(entries.ndim)]) for axis_at in (source, target)]
    chosen = jax.random.permutation(key, blocks)[partner]
    strong = (owner == chosen) | (owner == (partner + blocks // 2) % blocks)
    return jnp.where(strong, factor * entries, entries)


def block_scale(stream_key, dims, cuts, low, high):
    def one(dim, shards_of):
        steps = jax.random.uniform(jax.random.fold_in(jax.random.fold_in(stream_key, 6), dim), (shards_of,), jnp.float32, low / len(cuts), high / len(cuts))
        return jnp.repeat(jnp.exp(steps), dims[dim] // shards_of).reshape((-1,) + (1,) * (len(dims) - dim - 1))

    gain = one(*cuts[0])
    for cut in cuts[1:]:
        gain = gain * one(*cut)
    return gain


def gaussian(stream_key, shape, spread, most, shards=(), kind=jnp.bfloat16):
    drawn = spread * jax.random.normal(stream_key, shape, jnp.float32)
    if shards:
        drawn = drawn * block_scale(stream_key, shape, shards, -0.22, 0.18)
    return jnp.clip(drawn, -most, most).astype(kind)


def heavy_noise(key, dims, deviation, bound, shards, heavy, kind=jnp.bfloat16):
    values = deviation * jax.random.normal(key, dims, jnp.float32)
    if shards:
        values = values * block_scale(key, dims, shards, -0.22, 0.18)
    return jnp.clip(raised(values, jax.random.fold_in(key, 3), *heavy), -bound, bound).astype(kind)


def setup_inputs(seed: int = 0) -> dict:
    keys = jax.random.split(jax.random.key(seed), 9)
    lengths = draw_lengths(jax.random.fold_in(keys[8], 71), 0)
    page_table = draw_page_table(jax.random.fold_in(keys[8], 71), 0)
    migration = draw_migration(jax.random.fold_in(keys[8], 71), 0)
    dest_slots = draw_dest_slots(jax.random.fold_in(keys[8], 71), 0)
    queries = draw_queries(jax.random.fold_in(keys[8], 71), 0)
    key_cache = draw_key_cache(jax.random.fold_in(keys[8], 71), 0)
    value_cache = gaussian(keys[6], (N_INST, LAYERS, KVH, POOL * PAGE, HD), 1.0, 5.0, ((0, 2), (1, 8), (2, 8)))
    out_weight = heavy_noise(keys[7], (LAYERS, HEADS * HD, D), (HEADS * HD) ** -0.5, 0.09375, ((0, 8), (1, 8)), (1, 2, 8, 2.0))
    return dict(lengths=lengths, page_table=page_table, migration=migration, dest_slots=dest_slots, queries=queries, key_cache=key_cache, value_cache=value_cache, out_weight=out_weight)


def attend_all(query_rows, key_rows, value_rows, page_map, length_list):
    group_size = HEADS // KVH
    scale_factor = 1.0 / math.sqrt(HD)
    key_pages = key_rows.reshape(KVH, POOL, PAGE, HD)
    value_pages = value_rows.reshape(KVH, POOL, PAGE, HD)
    gathered_keys = key_pages[:, page_map].reshape(KVH, ROWS, MAXP * PAGE, HD).astype(jnp.float32)
    gathered_values = value_pages[:, page_map].reshape(KVH, ROWS, MAXP * PAGE, HD).astype(jnp.float32)
    query_split = query_rows.reshape(ROWS, KVH, group_size, HD).astype(jnp.float32)
    scores = jnp.einsum('rkgd,krtd->rkgt', query_split, gathered_keys, precision=lax.Precision.HIGHEST) * scale_factor
    position = jnp.arange(MAXP * PAGE, dtype=jnp.int32)
    visible = position[None, :] < length_list[:, None]
    scores = jnp.where(visible[:, None, None, :], scores, -jnp.inf)
    weights = jax.nn.softmax(scores, axis=-1)
    attended = jnp.einsum('rkgt,krtd->rkgd', weights, gathered_values, precision=lax.Precision.HIGHEST)
    return attended.reshape(ROWS, HEADS * HD).astype(jnp.bfloat16)

def reference(lengths, page_table, migration, dest_slots, queries, key_cache, value_cache, out_weight):

    def one_layer(flat_index):
        instance = flat_index // LAYERS
        layer_index = flat_index % LAYERS
        attended = attend_all(queries[instance, layer_index], key_cache[instance, layer_index], value_cache[instance, layer_index], page_table[instance], lengths[instance])
        return jnp.dot(attended, out_weight[layer_index], preferred_element_type=jnp.float32)
    layer_terms = lax.map(one_layer, jnp.arange(N_INST * LAYERS, dtype=jnp.int32))
    update = lax.optimization_barrier(jnp.sum(layer_terms.reshape(N_INST, LAYERS, ROWS, D), axis=1)).astype(jnp.bfloat16)
    movers = migration[:, 0]
    sources = migration[:, 1]
    targets = migration[:, 2]
    moved_lengths = lengths[sources, movers]
    live_pages = (jnp.arange(MAXP, dtype=jnp.int32)[None, :] * PAGE < moved_lengths[:, None]).reshape(-1)
    slot_ids = page_table[sources, movers].reshape(-1)
    source_rep = jnp.repeat(sources, MAXP)
    target_rep = jnp.repeat(targets, MAXP)
    recv_ids = dest_slots.reshape(-1)

    def place(cache_array):
        pages_all = cache_array.reshape(N_INST, LAYERS, KVH, POOL, PAGE, HD)
        moved_pages = pages_all[source_rep, :, :, slot_ids]
        areas = []
        for target in range(N_INST):
            keep = live_pages & (target_rep == target)
            kept = jnp.where(keep[:, None, None, None, None], moved_pages, jnp.zeros_like(moved_pages))
            areas.append(jnp.zeros((RECV, LAYERS, KVH, PAGE, HD), cache_array.dtype).at[recv_ids].set(kept))
        everything = jnp.stack(areas).transpose(0, 2, 3, 1, 4, 5)
        return everything.reshape(N_INST, LAYERS, KVH, RECV * PAGE, HD)
    return (update, place(key_cache), place(value_cache))
```

```python
import functools
import math

import jax
import jax.numpy as jnp
from jax import lax
from jax.experimental import pallas as pl
from jax.experimental.pallas import tpu as pltpu
from jax.sharding import PartitionSpec as P


PAGE = 128
GROUP = 8
CHUNK = 512

ANY = pl.BlockSpec(memory_space=pltpu.HBM)
SMEM = pl.BlockSpec(memory_space=pltpu.SMEM)
VMEM = pl.BlockSpec(memory_space=pltpu.VMEM)


def attend_kernel(
    rows, heads, pages,
    lengths, page_table, queries, keys, values, weight,
    out,
    q32, kbuf, vbuf, wbuf, attended, ksem, vsem, wsem,
):
    inst = lax.axis_index("inst")
    head_dim = keys.shape[1]
    blocks = rows // GROUP
    chunks = wbuf.shape[0]
    span = pages * PAGE
    scale = 1.0 / math.sqrt(head_dim)

    def fetch_pages(block):
        for g in range(GROUP):
            for p in range(pages):
                start = pl.multiple_of(page_table[p, 0, block * GROUP + g] * PAGE, PAGE)
                at = pl.ds((g * pages + p) * PAGE, PAGE)
                source = pl.ds(start, PAGE)
                pltpu.make_async_copy(keys.at[source], kbuf.at[block, at], ksem.at[block]).start()
                pltpu.make_async_copy(values.at[source], vbuf.at[block, at], vsem.at[block]).start()

    def weight_copy(chunk):
        at = pl.ds(pl.multiple_of(chunk * CHUNK, CHUNK), CHUNK)
        return pltpu.make_async_copy(weight.at[:, at], wbuf.at[chunk], wsem.at[chunk])

    fetch_pages(0)
    fetch_pages(1)
    q32[...] = queries[...].astype(jnp.float32)
    row_in_group = lax.broadcasted_iota(jnp.int32, (heads * GROUP, 1), 0) % GROUP
    token = lax.broadcasted_iota(jnp.int32, (heads * GROUP, span), 1)

    def attend_block(block, _):
        @pl.when(block + 2 < blocks)
        def _():
            fetch_pages(block + 2)

        for j in range(chunks // blocks):
            weight_copy(block * (chunks // blocks) + j).start()
        first = pl.multiple_of(block * GROUP, GROUP)
        q = q32[pl.ds(first, GROUP), :]
        q = jnp.concatenate(
            [q[:, h * head_dim : (h + 1) * head_dim] for h in range(heads)], axis=0
        ).astype(jnp.bfloat16)
        whole = pl.ds(0, GROUP * span)
        pltpu.make_async_copy(keys.at[whole], kbuf.at[block], ksem.at[block]).wait()
        scores = jnp.zeros((heads * GROUP, span), jnp.float32)
        limit = jnp.zeros((heads * GROUP, 1), jnp.int32)
        for g in range(GROUP):
            k = kbuf[block, g * span : (g + 1) * span, :]
            one = lax.dot_general(
                q, k, (((1,), (1,)), ((), ())), preferred_element_type=jnp.float32
            )
            mine = row_in_group == g
            scores = jnp.where(mine, one, scores)
            limit = jnp.where(mine, lengths[inst, block * GROUP + g], limit)
        scores = jnp.where(token < limit, scores, -1e30)
        top = jnp.max(scores, axis=1, keepdims=True)
        weights = jnp.exp((scores - top) * scale)
        total = jnp.sum(weights, axis=1, keepdims=True)
        weights = weights.astype(jnp.bfloat16)
        pltpu.make_async_copy(values.at[whole], vbuf.at[block], vsem.at[block]).wait()
        result = jnp.zeros((heads * GROUP, head_dim), jnp.float32)
        for g in range(GROUP):
            v = vbuf[block, g * span : (g + 1) * span, :]
            one = jnp.dot(weights, v, preferred_element_type=jnp.float32)
            result = jnp.where(row_in_group == g, one, result)
        result = result / total
        for h in range(heads):
            attended[pl.ds(first, GROUP), h * head_dim : (h + 1) * head_dim] = result[
                h * GROUP : (h + 1) * GROUP, :
            ]
        return 0

    lax.fori_loop(0, blocks, attend_block, 0)
    rounded = attended[...].astype(jnp.bfloat16)

    def project(chunk, _):
        weight_copy(chunk).wait()
        part = jnp.dot(rounded, wbuf[chunk], preferred_element_type=jnp.float32)
        width = out.shape[2]
        for j in range(CHUNK // width):
            out[chunk * (CHUNK // width) + j] = part[:, j * width : (j + 1) * width].astype(
                out.dtype
            )
        return 0

    lax.fori_loop(0, chunks, project, 0)


def attend_project(lengths, page_table, queries, keys, values, weight, parts):
    rows, width = queries.shape
    head_dim = keys.shape[1]
    heads = width // head_dim
    pages = page_table.shape[0]
    blocks = rows // GROUP
    depth, columns = weight.shape
    chunks = columns // CHUNK
    return pl.pallas_call(
        functools.partial(attend_kernel, rows, heads, pages),
        out_shape=jax.ShapeDtypeStruct((parts, rows, columns // parts), jnp.bfloat16),
        in_specs=[SMEM, SMEM, VMEM, ANY, ANY, ANY],
        out_specs=VMEM,
        scratch_shapes=[
            pltpu.VMEM((rows, width), jnp.float32),
            pltpu.VMEM((blocks, GROUP * pages * PAGE, head_dim), keys.dtype),
            pltpu.VMEM((blocks, GROUP * pages * PAGE, head_dim), values.dtype),
            pltpu.VMEM((chunks, depth, CHUNK), weight.dtype),
            pltpu.VMEM((rows, width), jnp.float32),
            pltpu.SemaphoreType.DMA((blocks,)),
            pltpu.SemaphoreType.DMA((blocks,)),
            pltpu.SemaphoreType.DMA((chunks,)),
        ],
        compiler_params=pltpu.CompilerParams(vmem_limit_bytes=60 * 1024 * 1024),
        cost_estimate=pl.CostEstimate(
            flops=2 * rows * depth * columns + 4 * rows * width * pages * PAGE,
            bytes_accessed=2 * (weight.size + 2 * keys.size),
            transcendentals=0,
        ),
        name="attend_project",
    )(lengths, page_table, queries, keys, values, weight)


def outgoing_kernel(moves, pages, lengths, page_table, migration, dest_slots, after, keys, values,
                    key_image, value_image, ksem, vsem):
    inst = lax.axis_index("inst")
    key_image[...] = jnp.zeros_like(key_image)
    value_image[...] = jnp.zeros_like(value_image)

    def each(act):
        for k in range(moves):
            move = (1 - inst) * moves + k
            request = migration[0, move]
            held = lengths[inst, request]
            for p in range(pages):
                source = pl.multiple_of(page_table[p, 0, request] * PAGE, PAGE)
                target = pl.multiple_of(dest_slots[p, move] * PAGE, PAGE)

                @pl.when(p * PAGE < held)
                def _():
                    for cache, image, sem in (
                        (keys, key_image, ksem), (values, value_image, vsem)
                    ):
                        act(
                            pltpu.make_async_copy(
                                cache.at[pl.ds(source, PAGE)],
                                image.at[pl.ds(target, PAGE)],
                                sem.at[k * pages + p],
                            )
                        )

    each(lambda copy: copy.start())
    each(lambda copy: copy.wait())


def outgoing(lengths, page_table, migration, dest_slots, after, keys, values):
    moves = migration.shape[1] // 2
    pages = page_table.shape[0]
    image = jax.ShapeDtypeStruct((dest_slots.size * PAGE, keys.shape[1]), keys.dtype)
    return pl.pallas_call(
        functools.partial(outgoing_kernel, moves, pages),
        out_shape=(image, image),
        in_specs=[SMEM, SMEM, SMEM, SMEM, ANY, ANY, ANY],
        out_specs=(VMEM, VMEM),
        scratch_shapes=[
            pltpu.SemaphoreType.DMA((moves * pages,)),
            pltpu.SemaphoreType.DMA((moves * pages,)),
        ],
        compiler_params=pltpu.CompilerParams(vmem_limit_bytes=60 * 1024 * 1024),
        cost_estimate=pl.CostEstimate(
            flops=1_000_000, bytes_accessed=3 * 2 * image.size, transcendentals=0
        ),
        name="outgoing",
    )(lengths, page_table, migration, dest_slots, after, keys, values)


def body(lengths, page_table, migration, dest_slots, queries, key_cache, value_cache, out_weight):
    page_table = jnp.transpose(page_table, (2, 0, 1))
    migration, dest_slots = migration.T, dest_slots.T
    parts = lax.axis_size("pipe") * lax.axis_size("tensor")
    keys = key_cache.reshape(key_cache.shape[3:])
    values = value_cache.reshape(value_cache.shape[3:])
    partial = attend_project(
        lengths, page_table, queries.reshape(queries.shape[2:]), keys, values,
        out_weight.reshape(out_weight.shape[1:]), parts,
    )
    arrived = lax.all_to_all(partial, ("pipe", "tensor"), split_axis=0, concat_axis=0, tiled=True)
    images = outgoing(lengths, page_table, migration, dest_slots, partial, keys, values)
    received = [lax.ppermute(image, "inst", [(0, 1), (1, 0)]) for image in images]
    update = arrived.astype(jnp.float32).sum(axis=0).astype(jnp.bfloat16)
    return (update[None], *[r.reshape(1, 1, 1, *r.shape) for r in received])


def solution(mesh):
    placed = (
        P(),
        P("inst", None, None),
        P(),
        P(),
        P("inst", "pipe", None, "tensor"),
        P("inst", "pipe", "tensor", None, None),
        P("inst", "pipe", "tensor", None, None),
        P("pipe", "tensor", None),
    )
    return jax.shard_map(
        body,
        mesh=mesh,
        in_specs=placed,
        out_specs=(
            P("inst", None, ("pipe", "tensor")),
            P("inst", "pipe", "tensor", None, None),
            P("inst", "pipe", "tensor", None, None),
        ),
        check_vma=False,
    )
```

```python
import functools
import math

import jax
import jax.numpy as jnp
from jax import lax
from jax.experimental import pallas as pl
from jax.experimental.pallas import tpu as pltpu
from jax.sharding import PartitionSpec as P


PAGE = 128
GROUP = 16
CHUNK = 512
LEAD = (3, 0, 0, 4, 4)

ATTEND_VMEM = 40
PACK_VMEM = 16

HBM = pl.BlockSpec(memory_space=pltpu.HBM)
SMEM = pl.BlockSpec(memory_space=pltpu.SMEM)
VMEM = pl.BlockSpec(memory_space=pltpu.VMEM)


def attend_kernel(
    pages,
    lengths_in, table_in, queries_in, keys, values, weight,
    out,
    lengths, page_table, queries, masked, kbuf, vbuf, wbuf, attended, staged,
    isem, qsem, ksem, vsem, wsem, osem,
):
    inst = lax.axis_index("inst")
    rows, width = queries.shape
    head_dim = keys.shape[1]
    heads = width // head_dim
    blocks = rows // GROUP
    chunks = wbuf.shape[0]
    stack = heads * GROUP
    scale = 1.0 / math.sqrt(head_dim)

    def fetch(cache, buffer, sem, block, held):
        for p in range(held):
            for g in range(GROUP):
                start = pl.multiple_of(page_table[p, 0, block * GROUP + g] * PAGE, PAGE)
                at = (block, pl.ds(p * PAGE, PAGE), pl.ds(g * head_dim, head_dim))
                pltpu.make_async_copy(
                    cache.at[pl.ds(start, PAGE)], buffer.at[at], sem.at[block]
                ).start()

    def weight_copy(chunk):
        at = pl.ds(pl.multiple_of(chunk * CHUNK, CHUNK), CHUNK)
        return pltpu.make_async_copy(weight.at[:, at], wbuf.at[chunk], wsem.at[chunk])

    def arrive(buffer, sem, block, held):
        at = (pl.ds(0, held * PAGE), pl.ds(0, GROUP * head_dim))
        pltpu.make_async_copy(weight.at[at], buffer.at[block, at[0]], sem.at[block]).wait()

    table_copy = pltpu.make_async_copy(table_in, page_table, isem.at[0])
    length_copy = pltpu.make_async_copy(lengths_in, lengths, isem.at[1])
    query_copy = pltpu.make_async_copy(queries_in, queries, qsem)
    table_copy.start()
    length_copy.start()
    query_copy.start()
    for j in range(LEAD[0]):
        weight_copy(j).start()
    row_in_group = lax.broadcasted_iota(jnp.int32, (stack, head_dim), 0) % GROUP
    lane_in_group = lax.broadcasted_iota(jnp.int32, (1, stack), 1) % GROUP

    def attend(held):
        token = lax.broadcasted_iota(jnp.int32, (held * PAGE, stack), 0)

        def score(block):
            q = queries[block * GROUP : (block + 1) * GROUP, :].astype(jnp.float32)
            q = jnp.concatenate(
                [q[:, h * head_dim : (h + 1) * head_dim] for h in range(heads)], axis=0
            )
            slot = block % 2
            for g in range(GROUP):
                masked[slot, :, g * head_dim : (g + 1) * head_dim] = jnp.where(
                    row_in_group == g, q, 0.0
                ).astype(masked.dtype)
            return lax.dot_general(
                kbuf[block, : held * PAGE], masked[slot], (((1,), (1,)), ((), ())),
                preferred_element_type=jnp.float32,
            )

        def finish(block, scores):
            limit = jnp.zeros((1, stack), jnp.int32)
            for g in range(GROUP):
                limit = jnp.where(lane_in_group == g, lengths[inst, block * GROUP + g], limit)
            scores = jnp.where(token < limit, scores, -1e30)
            top = jnp.max(scores, axis=0, keepdims=True)
            weights = jnp.exp((scores - top) * scale)
            share = 1.0 / jnp.sum(weights, axis=0, keepdims=True)
            share = jnp.broadcast_to(share, (head_dim, stack)).T
            weights = weights.T.astype(jnp.bfloat16)
            result = jnp.zeros((stack, head_dim), jnp.float32)
            for g in range(0, GROUP, 2):
                pair = jnp.dot(
                    weights, vbuf[block, : held * PAGE, g * head_dim : (g + 2) * head_dim],
                    preferred_element_type=jnp.float32,
                )
                result = jnp.where(row_in_group == g, pair[:, :head_dim], result)
                result = jnp.where(row_in_group == g + 1, pair[:, head_dim:], result)
            result = result * share
            for h in range(heads):
                attended[
                    block * GROUP : (block + 1) * GROUP, h * head_dim : (h + 1) * head_dim
                ] = result[h * GROUP : (h + 1) * GROUP, :].astype(attended.dtype)

        fetch(keys, kbuf, ksem, 0, held)
        fetch(values, vbuf, vsem, 0, held)
        fetch(keys, kbuf, ksem, 1, held)
        fetch(values, vbuf, vsem, 1, held)
        length_copy.wait()
        query_copy.wait()
        arrive(kbuf, ksem, 0, held)
        scores = score(0)
        for block in range(blocks):
            if block + 2 < blocks:
                fetch(keys, kbuf, ksem, block + 2, held)
                fetch(values, vbuf, vsem, block + 2, held)
            for j in range(sum(LEAD[: block + 1]), sum(LEAD[: block + 2])):
                weight_copy(j).start()
            arrive(vbuf, vsem, block, held)
            if block + 1 < blocks:
                arrive(kbuf, ksem, block + 1, held)
                following = score(block + 1)
            finish(block, scores)
            scores = following

    table_copy.wait()

    @pl.when(inst == 0)
    def _():
        attend(pages - 1)

    @pl.when(inst != 0)
    def _():
        attend(pages)

    piece = out.shape[2]
    per_chunk = CHUNK // piece

    def store(chunk):
        at = pl.ds(chunk * per_chunk, per_chunk)
        return pltpu.make_async_copy(staged.at[at], out.at[at], osem.at[chunk])

    def project(chunk, _):
        @pl.when(chunk + sum(LEAD) < chunks)
        def _():
            weight_copy(chunk + sum(LEAD)).start()

        weight_copy(chunk).wait()
        part = jnp.dot(attended[...], wbuf[chunk], preferred_element_type=jnp.float32)
        for j in range(per_chunk):
            staged[chunk * per_chunk + j] = part[:, j * piece : (j + 1) * piece].astype(
                out.dtype
            )
        store(chunk).start()
        return 0

    lax.fori_loop(0, chunks, project, 0)
    lax.fori_loop(0, chunks, lambda chunk, _: (store(chunk).wait(), 0)[1], 0)


def attend_project(lengths, page_table, queries, keys, values, weight, parts):
    rows, width = queries.shape
    head_dim = keys.shape[1]
    pages = page_table.shape[0]
    blocks = rows // GROUP
    depth, columns = weight.shape
    chunks = columns // CHUNK
    cache = pltpu.VMEM((blocks, pages * PAGE, GROUP * head_dim), keys.dtype)
    return pl.pallas_call(
        functools.partial(attend_kernel, pages),
        out_shape=jax.ShapeDtypeStruct((parts, rows, columns // parts), jnp.bfloat16),
        in_specs=[HBM] * 6,
        out_specs=HBM,
        scratch_shapes=[
            pltpu.SMEM(lengths.shape, jnp.int32),
            pltpu.SMEM(page_table.shape, jnp.int32),
            pltpu.VMEM(queries.shape, queries.dtype),
            pltpu.VMEM((2, width // head_dim * GROUP, GROUP * head_dim), queries.dtype),
            cache,
            cache,
            pltpu.VMEM((chunks, depth, CHUNK), weight.dtype),
            pltpu.VMEM((rows, width), jnp.bfloat16),
            pltpu.VMEM((parts, rows, columns // parts), jnp.bfloat16),
            pltpu.SemaphoreType.DMA((2,)),
            pltpu.SemaphoreType.DMA,
            pltpu.SemaphoreType.DMA((blocks,)),
            pltpu.SemaphoreType.DMA((blocks,)),
            pltpu.SemaphoreType.DMA((chunks,)),
            pltpu.SemaphoreType.DMA((chunks,)),
        ],
        compiler_params=pltpu.CompilerParams(vmem_limit_bytes=ATTEND_VMEM * 1024 * 1024),
        cost_estimate=pl.CostEstimate(
            flops=2 * rows * depth * columns + 4 * rows * width * pages * PAGE,
            bytes_accessed=2 * (weight.size + 2 * keys.size),
            transcendentals=0,
        ),
        name="attend_project",
    )(lengths, page_table, queries, keys, values, weight)


def pack_kernel(page_table, migration, keys, values, packed, sem):
    moves = migration.shape[1] // 2
    pages = page_table.shape[0]
    first = (1 - lax.axis_index("inst")) * moves
    half = packed.shape[0] // 2
    for k in range(moves):
        request = migration[0, first + k]
        for p in range(pages):
            source = pl.ds(pl.multiple_of(page_table[p, 0, request] * PAGE, PAGE), PAGE)
            at = (k * pages + p) * PAGE
            pltpu.make_async_copy(keys.at[source], packed.at[pl.ds(at, PAGE)], sem).start()
            pltpu.make_async_copy(
                values.at[source], packed.at[pl.ds(half + at, PAGE)], sem
            ).start()
    pltpu.make_async_copy(keys.at[pl.ds(0, 2 * half)], packed, sem).wait()


def pack(page_table, migration, keys, values):
    slots = migration.shape[1] // 2 * page_table.shape[0]
    packed = jax.ShapeDtypeStruct((2 * slots * PAGE, keys.shape[1]), keys.dtype)
    return pl.pallas_call(
        pack_kernel,
        out_shape=pltpu.VMEM(packed.shape, packed.dtype),
        in_specs=[SMEM, SMEM, HBM, HBM],
        out_specs=VMEM,
        scratch_shapes=[pltpu.SemaphoreType.DMA],
        compiler_params=pltpu.CompilerParams(vmem_limit_bytes=PACK_VMEM * 1024 * 1024),
        cost_estimate=pl.CostEstimate(
            flops=1_000_000, bytes_accessed=4 * packed.size, transcendentals=0
        ),
        name="pack",
    )(page_table, migration, keys, values)


def place_kernel(lengths, migration, dest_slots, packed, key_area, value_area, blank, ksem, vsem):
    inst = lax.axis_index("inst")
    pages, moves = dest_slots.shape
    half = packed.shape[0] // 2
    blank[...] = jnp.zeros_like(blank)
    for m in range(moves):
        from_inst = 1 if m < moves // 2 else 0
        held = lengths[from_inst, migration[0, m]]
        for p in range(pages):
            target = pl.ds(pl.multiple_of(dest_slots[p, m] * PAGE, PAGE), PAGE)
            at = (m % (moves // 2) * pages + p) * PAGE
            live = (inst != from_inst) & (p * PAGE < held)
            for area, sem, offset in ((key_area, ksem, at), (value_area, vsem, half + at)):

                @pl.when(live)
                def _():
                    pltpu.make_async_copy(
                        packed.at[pl.ds(offset, PAGE)], area.at[target], sem
                    ).start()

                @pl.when(jnp.logical_not(live))
                def _():
                    pltpu.make_async_copy(blank, area.at[target], sem).start()

    for area, sem in ((key_area, ksem), (value_area, vsem)):
        pltpu.make_async_copy(area, area, sem).wait()


def place(lengths, migration, dest_slots, packed):
    area = jax.ShapeDtypeStruct((dest_slots.size * PAGE, packed.shape[1]), packed.dtype)
    return pl.pallas_call(
        place_kernel,
        out_shape=(area, area),
        in_specs=[SMEM, SMEM, SMEM, VMEM],
        out_specs=(HBM, HBM),
        scratch_shapes=[
            pltpu.VMEM((PAGE, packed.shape[1]), packed.dtype),
            pltpu.SemaphoreType.DMA,
            pltpu.SemaphoreType.DMA,
        ],
        compiler_params=pltpu.CompilerParams(vmem_limit_bytes=PACK_VMEM * 1024 * 1024),
        cost_estimate=pl.CostEstimate(
            flops=1_000_000, bytes_accessed=4 * area.size, transcendentals=0
        ),
        name="place",
    )(lengths, migration, dest_slots, packed)


def body(lengths, page_table, migration, dest_slots, queries, key_cache, value_cache, out_weight):
    parts = lax.axis_size("pipe") * lax.axis_size("tensor")
    (lengths, page_table, migration, dest_slots, queries, keys, values, weight) = [
        pltpu.with_memory_space_constraint(array, pltpu.HBM)
        for array in (
            lengths,
            jnp.transpose(page_table, (2, 0, 1)),
            migration.T,
            dest_slots.T,
            queries.reshape(queries.shape[2:]),
            key_cache.reshape(key_cache.shape[3:]),
            value_cache.reshape(value_cache.shape[3:]),
            out_weight.reshape(out_weight.shape[1:]),
        )
    ]
    partial = attend_project(lengths, page_table, queries, keys, values, weight, parts)
    arrived = lax.all_to_all(partial, ("pipe", "tensor"), split_axis=0, concat_axis=0, tiled=True)
    packed = pack(page_table, migration, keys, values)
    moved = lax.ppermute(packed, "inst", [(0, 1), (1, 0)])
    received = place(lengths, migration, dest_slots, moved)
    update = arrived.astype(jnp.float32).sum(axis=0).astype(jnp.bfloat16)
    return (update[None], *[r.reshape(1, 1, 1, *r.shape) for r in received])


def solution(mesh):
    placed = (
        P(),
        P("inst", None, None),
        P(),
        P(),
        P("inst", "pipe", None, "tensor"),
        P("inst", "pipe", "tensor", None, None),
        P("inst", "pipe", "tensor", None, None),
        P("pipe", "tensor", None),
    )
    return jax.shard_map(
        body,
        mesh=mesh,
        in_specs=placed,
        out_specs=(
            P("inst", None, ("pipe", "tensor")),
            P("inst", "pipe", "tensor", None, None),
            P("inst", "pipe", "tensor", None, None),
        ),
        check_vma=False,
    )
```

```python
import functools
import math

import jax
import jax.numpy as jnp
from jax import lax
from jax.experimental import pallas as pl
from jax.experimental.pallas import tpu as pltpu
from jax.sharding import PartitionSpec as P


PAGE = 128
GROUP = 16
CHUNK = 1024
LEAD = (0, 0, 1, 2, 2)
KEY_COPIES = 8

ATTEND_VMEM = 40
PACK_VMEM = 16

HBM = pl.BlockSpec(memory_space=pltpu.HBM)
SMEM = pl.BlockSpec(memory_space=pltpu.SMEM)
VMEM = pl.BlockSpec(memory_space=pltpu.VMEM)


def attend_kernel(
    pages,
    lengths_in, table_in, queries_in, keys, values, weight,
    out,
    lengths, page_table, queries, kbuf, vbuf, wbuf, attended, staged,
    isem, qsem, ksem, vsem, wsem, osem,
):
    inst = lax.axis_index("inst")
    rows, width = queries.shape
    head_dim = keys.shape[1]
    heads = width // head_dim
    blocks = rows // GROUP
    chunks = wbuf.shape[0]
    stack = heads * GROUP
    scale = 1.0 / math.sqrt(head_dim)

    def page(p, request):
        return pl.ds(pl.multiple_of(page_table[p, 0, request] * PAGE, PAGE), PAGE)

    def fetch_values(block, held):
        for p in range(held):
            for g in range(GROUP):
                at = (block, pl.ds(p * PAGE, PAGE), pl.ds(g * head_dim, head_dim))
                pltpu.make_async_copy(
                    values.at[page(p, block * GROUP + g)], vbuf.at[at], vsem.at[block]
                ).start()

    def weight_copy(chunk):
        at = pl.ds(pl.multiple_of(chunk * CHUNK, CHUNK), CHUNK)
        return pltpu.make_async_copy(weight.at[:, at], wbuf.at[chunk], wsem.at[chunk])

    def values_arrive(block, held):
        at = (pl.ds(0, held * PAGE), pl.ds(0, GROUP * head_dim))
        pltpu.make_async_copy(weight.at[at], vbuf.at[block, at[0]], vsem.at[block]).wait()

    def key_copy(part):
        at = pl.ds(part * (keys.shape[0] // KEY_COPIES), keys.shape[0] // KEY_COPIES)
        return pltpu.make_async_copy(keys.at[at], kbuf.at[at], ksem.at[part])

    table_copy = pltpu.make_async_copy(table_in, page_table, isem.at[0])
    length_copy = pltpu.make_async_copy(lengths_in, lengths, isem.at[1])
    query_copy = pltpu.make_async_copy(queries_in, queries, qsem)
    table_copy.start()
    length_copy.start()
    query_copy.start()
    for part in range(KEY_COPIES):
        key_copy(part).start()
    for j in range(LEAD[0]):
        weight_copy(j).start()
    row_in_group = lax.broadcasted_iota(jnp.int32, (stack, head_dim), 0) % GROUP
    lane_in_group = lax.broadcasted_iota(jnp.int32, (1, stack), 1) % GROUP

    def attend(held):
        token = lax.broadcasted_iota(jnp.int32, (held * PAGE, stack), 0)

        def score(block):
            q = queries[block * GROUP : (block + 1) * GROUP, :].astype(jnp.float32)
            q = jnp.concatenate(
                [q[:, h * head_dim : (h + 1) * head_dim] for h in range(heads)], axis=0
            )
            total = None
            for g in range(0, GROUP, 2):
                pair = jnp.concatenate(
                    [jnp.where(row_in_group == g + e, q, 0.0) for e in range(2)], axis=1
                ).astype(jnp.bfloat16)
                k = jnp.concatenate(
                    [
                        jnp.concatenate(
                            [kbuf[page(p, block * GROUP + g + e), :] for e in range(2)], axis=1
                        )
                        for p in range(held)
                    ],
                    axis=0,
                )
                part = lax.dot_general(
                    k, pair, (((1,), (1,)), ((), ())), preferred_element_type=jnp.float32
                )
                total = part if total is None else total + part
            return total

        def finish(block, scores):
            limit = jnp.zeros((1, stack), jnp.int32)
            for g in range(GROUP):
                limit = jnp.where(lane_in_group == g, lengths[inst, block * GROUP + g], limit)
            scores = jnp.where(token < limit, scores, -1e30)
            top = jnp.max(scores, axis=0, keepdims=True)
            weights = jnp.exp((scores - top) * scale)
            share = 1.0 / jnp.sum(weights, axis=0, keepdims=True)
            share = jnp.broadcast_to(share, (head_dim, stack)).T
            weights = weights.T.astype(jnp.bfloat16)
            result = jnp.zeros((stack, head_dim), jnp.float32)
            for g in range(0, GROUP, 2):
                pair = jnp.dot(
                    weights, vbuf[block, : held * PAGE, g * head_dim : (g + 2) * head_dim],
                    preferred_element_type=jnp.float32,
                )
                result = jnp.where(row_in_group == g, pair[:, :head_dim], result)
                result = jnp.where(row_in_group == g + 1, pair[:, head_dim:], result)
            result = result * share
            for h in range(heads):
                attended[
                    block * GROUP : (block + 1) * GROUP, h * head_dim : (h + 1) * head_dim
                ] = result[h * GROUP : (h + 1) * GROUP, :].astype(attended.dtype)

        fetch_values(0, held)
        fetch_values(1, held)
        length_copy.wait()
        query_copy.wait()
        for part in range(KEY_COPIES):
            key_copy(part).wait()
        scores = score(0)
        for block in range(blocks):
            if block + 2 < blocks:
                fetch_values(block + 2, held)
            for j in range(sum(LEAD[: block + 1]), sum(LEAD[: block + 2])):
                weight_copy(j).start()
            values_arrive(block, held)
            if block + 1 < blocks:
                following = score(block + 1)
            finish(block, scores)
            scores = following

    table_copy.wait()

    @pl.when(inst == 0)
    def _():
        attend(pages - 1)

    @pl.when(inst != 0)
    def _():
        attend(pages)

    piece = out.shape[2]
    per_chunk = CHUNK // piece

    def store(chunk):
        at = pl.ds(chunk * per_chunk, per_chunk)
        return pltpu.make_async_copy(staged.at[at], out.at[at], osem.at[chunk])

    def project(chunk, _):
        @pl.when(chunk + sum(LEAD) < chunks)
        def _():
            weight_copy(chunk + sum(LEAD)).start()

        weight_copy(chunk).wait()
        part = jnp.dot(attended[...], wbuf[chunk], preferred_element_type=jnp.float32)
        for j in range(per_chunk):
            staged[chunk * per_chunk + j] = part[:, j * piece : (j + 1) * piece].astype(
                out.dtype
            )
        store(chunk).start()
        return 0

    lax.fori_loop(0, chunks, project, 0)
    lax.fori_loop(0, chunks, lambda chunk, _: (store(chunk).wait(), 0)[1], 0)


def attend_project(lengths, page_table, queries, keys, values, weight, parts):
    rows, width = queries.shape
    head_dim = keys.shape[1]
    pages = page_table.shape[0]
    blocks = rows // GROUP
    depth, columns = weight.shape
    chunks = columns // CHUNK
    return pl.pallas_call(
        functools.partial(attend_kernel, pages),
        out_shape=jax.ShapeDtypeStruct((parts, rows, columns // parts), jnp.bfloat16),
        in_specs=[HBM] * 6,
        out_specs=HBM,
        scratch_shapes=[
            pltpu.SMEM(lengths.shape, jnp.int32),
            pltpu.SMEM(page_table.shape, jnp.int32),
            pltpu.VMEM(queries.shape, queries.dtype),
            pltpu.VMEM(keys.shape, keys.dtype),
            pltpu.VMEM((blocks, pages * PAGE, GROUP * head_dim), values.dtype),
            pltpu.VMEM((chunks, depth, CHUNK), weight.dtype),
            pltpu.VMEM((rows, width), jnp.bfloat16),
            pltpu.VMEM((parts, rows, columns // parts), jnp.bfloat16),
            pltpu.SemaphoreType.DMA((2,)),
            pltpu.SemaphoreType.DMA,
            pltpu.SemaphoreType.DMA((KEY_COPIES,)),
            pltpu.SemaphoreType.DMA((blocks,)),
            pltpu.SemaphoreType.DMA((chunks,)),
            pltpu.SemaphoreType.DMA((chunks,)),
        ],
        compiler_params=pltpu.CompilerParams(vmem_limit_bytes=ATTEND_VMEM * 1024 * 1024),
        cost_estimate=pl.CostEstimate(
            flops=2 * rows * depth * columns + 4 * rows * width * pages * PAGE,
            bytes_accessed=2 * (weight.size + 2 * keys.size),
            transcendentals=0,
        ),
        name="attend_project",
    )(lengths, page_table, queries, keys, values, weight)


def pack_kernel(page_table, migration, keys, values, packed, sem):
    moves = migration.shape[1] // 2
    pages = page_table.shape[0]
    first = (1 - lax.axis_index("inst")) * moves
    half = packed.shape[0] // 2
    for k in range(moves):
        request = migration[0, first + k]
        for p in range(pages):
            source = pl.ds(pl.multiple_of(page_table[p, 0, request] * PAGE, PAGE), PAGE)
            at = (k * pages + p) * PAGE
            pltpu.make_async_copy(keys.at[source], packed.at[pl.ds(at, PAGE)], sem).start()
            pltpu.make_async_copy(
                values.at[source], packed.at[pl.ds(half + at, PAGE)], sem
            ).start()
    pltpu.make_async_copy(keys.at[pl.ds(0, 2 * half)], packed, sem).wait()


def pack(page_table, migration, keys, values):
    slots = migration.shape[1] // 2 * page_table.shape[0]
    packed = jax.ShapeDtypeStruct((2 * slots * PAGE, keys.shape[1]), keys.dtype)
    return pl.pallas_call(
        pack_kernel,
        out_shape=pltpu.VMEM(packed.shape, packed.dtype),
        in_specs=[SMEM, SMEM, HBM, HBM],
        out_specs=VMEM,
        scratch_shapes=[pltpu.SemaphoreType.DMA],
        compiler_params=pltpu.CompilerParams(vmem_limit_bytes=PACK_VMEM * 1024 * 1024),
        cost_estimate=pl.CostEstimate(
            flops=1_000_000, bytes_accessed=4 * packed.size, transcendentals=0
        ),
        name="pack",
    )(page_table, migration, keys, values)


def place_kernel(lengths, migration, dest_slots, packed, key_area, value_area, blank, ksem, vsem):
    inst = lax.axis_index("inst")
    pages, moves = dest_slots.shape
    half = packed.shape[0] // 2
    blank[...] = jnp.zeros_like(blank)
    for m in range(moves):
        from_inst = 1 if m < moves // 2 else 0
        held = lengths[from_inst, migration[0, m]]
        for p in range(pages):
            target = pl.ds(pl.multiple_of(dest_slots[p, m] * PAGE, PAGE), PAGE)
            at = (m % (moves // 2) * pages + p) * PAGE
            live = (inst != from_inst) & (p * PAGE < held)
            for area, sem, offset in ((key_area, ksem, at), (value_area, vsem, half + at)):

                @pl.when(live)
                def _():
                    pltpu.make_async_copy(
                        packed.at[pl.ds(offset, PAGE)], area.at[target], sem
                    ).start()

                @pl.when(jnp.logical_not(live))
                def _():
                    pltpu.make_async_copy(blank, area.at[target], sem).start()

    for area, sem in ((key_area, ksem), (value_area, vsem)):
        pltpu.make_async_copy(area, area, sem).wait()


def place(lengths, migration, dest_slots, packed):
    area = jax.ShapeDtypeStruct((dest_slots.size * PAGE, packed.shape[1]), packed.dtype)
    return pl.pallas_call(
        place_kernel,
        out_shape=(area, area),
        in_specs=[SMEM, SMEM, SMEM, VMEM],
        out_specs=(HBM, HBM),
        scratch_shapes=[
            pltpu.VMEM((PAGE, packed.shape[1]), packed.dtype),
            pltpu.SemaphoreType.DMA,
            pltpu.SemaphoreType.DMA,
        ],
        compiler_params=pltpu.CompilerParams(vmem_limit_bytes=PACK_VMEM * 1024 * 1024),
        cost_estimate=pl.CostEstimate(
            flops=1_000_000, bytes_accessed=4 * area.size, transcendentals=0
        ),
        name="place",
    )(lengths, migration, dest_slots, packed)


def body(lengths, page_table, migration, dest_slots, queries, key_cache, value_cache, out_weight):
    parts = lax.axis_size("pipe") * lax.axis_size("tensor")
    (lengths, page_table, migration, dest_slots, queries, keys, values, weight) = [
        pltpu.with_memory_space_constraint(array, pltpu.HBM)
        for array in (
            lengths,
            jnp.transpose(page_table, (2, 0, 1)),
            migration.T,
            dest_slots.T,
            queries.reshape(queries.shape[2:]),
            key_cache.reshape(key_cache.shape[3:]),
            value_cache.reshape(value_cache.shape[3:]),
            out_weight.reshape(out_weight.shape[1:]),
        )
    ]
    partial = attend_project(lengths, page_table, queries, keys, values, weight, parts)
    arrived = lax.all_to_all(partial, ("pipe", "tensor"), split_axis=0, concat_axis=0, tiled=True)
    packed = pack(page_table, migration, keys, values)
    moved = lax.ppermute(packed, "inst", [(0, 1), (1, 0)])
    received = place(lengths, migration, dest_slots, moved)
    update = arrived.astype(jnp.float32).sum(axis=0).astype(jnp.bfloat16)
    return (update[None], *[r.reshape(1, 1, 1, *r.shape) for r in received])


def solution(mesh):
    placed = (
        P(),
        P("inst", None, None),
        P(),
        P(),
        P("inst", "pipe", None, "tensor"),
        P("inst", "pipe", "tensor", None, None),
        P("inst", "pipe", "tensor", None, None),
        P("pipe", "tensor", None),
    )
    return jax.shard_map(
        body,
        mesh=mesh,
        in_specs=placed,
        out_specs=(
            P("inst", None, ("pipe", "tensor")),
            P("inst", "pipe", "tensor", None, None),
            P("inst", "pipe", "tensor", None, None),
        ),
        check_vma=False,
    )
```

```python
import functools
import math

import jax
import jax.numpy as jnp
from jax import lax
from jax.experimental import pallas as pl
from jax.experimental.pallas import tpu as pltpu
from jax.sharding import PartitionSpec as P


PAGE = 128
GROUP = 16
CHUNK = 1024
LEAD = (0, 0, 1, 2, 2)
KEY_COPIES = 8

ATTEND_VMEM = 40
PACK_VMEM = 16

HBM = pl.BlockSpec(memory_space=pltpu.HBM)
SMEM = pl.BlockSpec(memory_space=pltpu.SMEM)
VMEM = pl.BlockSpec(memory_space=pltpu.VMEM)


def attend_kernel(
    pages,
    lengths_in, table_in, queries_in, keys, values, weight,
    out,
    lengths, page_table, queries, kbuf, vbuf, wbuf, attended, staged,
    isem, qsem, ksem, vsem, wsem, osem,
):
    inst = lax.axis_index("inst")
    rows, width = queries.shape
    head_dim = keys.shape[1]
    heads = width // head_dim
    blocks = rows // GROUP
    chunks = wbuf.shape[0]
    stack = heads * GROUP
    scale = 1.0 / math.sqrt(head_dim)

    def page(p, request):
        return pl.ds(pl.multiple_of(page_table[p, 0, request] * PAGE, PAGE), PAGE)

    def fetch_values(block, held):
        for p in range(held):
            for g in range(GROUP):
                at = (block, pl.ds(p * PAGE, PAGE), pl.ds(g * head_dim, head_dim))
                pltpu.make_async_copy(
                    values.at[page(p, block * GROUP + g)], vbuf.at[at], vsem.at[block]
                ).start()

    def weight_copy(chunk):
        at = pl.ds(pl.multiple_of(chunk * CHUNK, CHUNK), CHUNK)
        return pltpu.make_async_copy(weight.at[:, at], wbuf.at[chunk], wsem.at[chunk])

    def values_arrive(block, held):
        at = (pl.ds(0, held * PAGE), pl.ds(0, GROUP * head_dim))
        pltpu.make_async_copy(weight.at[at], vbuf.at[block, at[0]], vsem.at[block]).wait()

    def key_copy(part):
        at = pl.ds(part * (keys.shape[0] // KEY_COPIES), keys.shape[0] // KEY_COPIES)
        return pltpu.make_async_copy(keys.at[at], kbuf.at[at], ksem.at[part])

    table_copy = pltpu.make_async_copy(table_in, page_table, isem.at[0])
    length_copy = pltpu.make_async_copy(lengths_in, lengths, isem.at[1])
    query_copy = pltpu.make_async_copy(queries_in, queries, qsem)
    table_copy.start()
    length_copy.start()
    query_copy.start()
    for part in range(KEY_COPIES):
        key_copy(part).start()
    for j in range(LEAD[0]):
        weight_copy(j).start()
    row_in_group = lax.broadcasted_iota(jnp.int32, (stack, head_dim), 0) % GROUP
    lane_in_group = lax.broadcasted_iota(jnp.int32, (1, stack), 1) % GROUP

    def attend(held):
        token = lax.broadcasted_iota(jnp.int32, (held * PAGE, stack), 0)

        def score(block):
            q = queries[block * GROUP : (block + 1) * GROUP, :].astype(jnp.float32)
            q = jnp.concatenate(
                [q[:, h * head_dim : (h + 1) * head_dim] for h in range(heads)], axis=0
            )
            total = None
            for g in range(0, GROUP, 2):
                pair = jnp.concatenate(
                    [jnp.where(row_in_group == g + e, q, 0.0) for e in range(2)], axis=1
                ).astype(jnp.bfloat16)
                k = jnp.concatenate(
                    [
                        jnp.concatenate(
                            [kbuf[page(p, block * GROUP + g + e), :] for e in range(2)], axis=1
                        )
                        for p in range(held)
                    ],
                    axis=0,
                )
                part = lax.dot_general(
                    k, pair, (((1,), (1,)), ((), ())), preferred_element_type=jnp.float32
                )
                total = part if total is None else total + part
            return total

        def finish(block, scores):
            limit = jnp.zeros((1, stack), jnp.int32)
            for g in range(GROUP):
                limit = jnp.where(lane_in_group == g, lengths[inst, block * GROUP + g], limit)
            scores = jnp.where(token < limit, scores, -1e30)
            top = jnp.max(scores, axis=0, keepdims=True)
            weights = jnp.exp((scores - top) * scale)
            share = 1.0 / jnp.sum(weights, axis=0, keepdims=True)
            share = jnp.broadcast_to(share, (head_dim, stack)).T
            weights = weights.T.astype(jnp.bfloat16)
            result = jnp.zeros((stack, head_dim), jnp.float32)
            for g in range(0, GROUP, 2):
                pair = jnp.dot(
                    weights, vbuf[block, : held * PAGE, g * head_dim : (g + 2) * head_dim],
                    preferred_element_type=jnp.float32,
                )
                result = jnp.where(row_in_group == g, pair[:, :head_dim], result)
                result = jnp.where(row_in_group == g + 1, pair[:, head_dim:], result)
            result = result * share
            for h in range(heads):
                attended[
                    block * GROUP : (block + 1) * GROUP, h * head_dim : (h + 1) * head_dim
                ] = result[h * GROUP : (h + 1) * GROUP, :].astype(attended.dtype)

        fetch_values(0, held)
        fetch_values(1, held)
        length_copy.wait()
        query_copy.wait()
        for part in range(KEY_COPIES):
            key_copy(part).wait()
        scores = score(0)
        for block in range(blocks):
            if block + 2 < blocks:
                fetch_values(block + 2, held)
            for j in range(sum(LEAD[: block + 1]), sum(LEAD[: block + 2])):
                weight_copy(j).start()
            values_arrive(block, held)
            if block + 1 < blocks:
                following = score(block + 1)
            finish(block, scores)
            scores = following

    table_copy.wait()

    @pl.when(inst == 0)
    def _():
        attend(pages - 1)

    @pl.when(inst != 0)
    def _():
        attend(pages)

    piece = out.shape[2]
    per_chunk = CHUNK // piece

    def store(chunk):
        at = pl.ds(chunk * per_chunk, per_chunk)
        return pltpu.make_async_copy(staged.at[at], out.at[at], osem.at[chunk])

    def project(chunk):
        if chunk + sum(LEAD) < chunks:
            weight_copy(chunk + sum(LEAD)).start()
        weight_copy(chunk).wait()
        part = jnp.dot(attended[...], wbuf[chunk], preferred_element_type=jnp.float32)
        for j in range(per_chunk):
            staged[chunk * per_chunk + j] = part[:, j * piece : (j + 1) * piece].astype(
                out.dtype
            )
        store(chunk).start()

    for chunk in range(chunks):
        project(chunk)
    lax.fori_loop(0, chunks, lambda chunk, _: (store(chunk).wait(), 0)[1], 0)


def attend_project(lengths, page_table, queries, keys, values, weight, parts):
    rows, width = queries.shape
    head_dim = keys.shape[1]
    pages = page_table.shape[0]
    blocks = rows // GROUP
    depth, columns = weight.shape
    chunks = columns // CHUNK
    return pl.pallas_call(
        functools.partial(attend_kernel, pages),
        out_shape=jax.ShapeDtypeStruct((parts, rows, columns // parts), jnp.bfloat16),
        in_specs=[HBM] * 6,
        out_specs=HBM,
        scratch_shapes=[
            pltpu.SMEM(lengths.shape, jnp.int32),
            pltpu.SMEM(page_table.shape, jnp.int32),
            pltpu.VMEM(queries.shape, queries.dtype),
            pltpu.VMEM(keys.shape, keys.dtype),
            pltpu.VMEM((blocks, pages * PAGE, GROUP * head_dim), values.dtype),
            pltpu.VMEM((chunks, depth, CHUNK), weight.dtype),
            pltpu.VMEM((rows, width), jnp.bfloat16),
            pltpu.VMEM((parts, rows, columns // parts), jnp.bfloat16),
            pltpu.SemaphoreType.DMA((2,)),
            pltpu.SemaphoreType.DMA,
            pltpu.SemaphoreType.DMA((KEY_COPIES,)),
            pltpu.SemaphoreType.DMA((blocks,)),
            pltpu.SemaphoreType.DMA((chunks,)),
            pltpu.SemaphoreType.DMA((chunks,)),
        ],
        compiler_params=pltpu.CompilerParams(vmem_limit_bytes=ATTEND_VMEM * 1024 * 1024),
        cost_estimate=pl.CostEstimate(
            flops=2 * rows * depth * columns + 4 * rows * width * pages * PAGE,
            bytes_accessed=2 * (weight.size + 2 * keys.size),
            transcendentals=0,
        ),
        name="attend_project",
    )(lengths, page_table, queries, keys, values, weight)


def pack_kernel(page_table, migration, keys, values, packed, sem):
    moves = migration.shape[1] // 2
    pages = page_table.shape[0]
    first = (1 - lax.axis_index("inst")) * moves
    half = packed.shape[0] // 2
    for k in range(moves):
        request = migration[0, first + k]
        for p in range(pages):
            source = pl.ds(pl.multiple_of(page_table[p, 0, request] * PAGE, PAGE), PAGE)
            at = (k * pages + p) * PAGE
            pltpu.make_async_copy(keys.at[source], packed.at[pl.ds(at, PAGE)], sem).start()
            pltpu.make_async_copy(
                values.at[source], packed.at[pl.ds(half + at, PAGE)], sem
            ).start()
    pltpu.make_async_copy(keys.at[pl.ds(0, 2 * half)], packed, sem).wait()


def pack(page_table, migration, keys, values):
    slots = migration.shape[1] // 2 * page_table.shape[0]
    packed = jax.ShapeDtypeStruct((2 * slots * PAGE, keys.shape[1]), keys.dtype)
    return pl.pallas_call(
        pack_kernel,
        out_shape=pltpu.VMEM(packed.shape, packed.dtype),
        in_specs=[SMEM, SMEM, HBM, HBM],
        out_specs=VMEM,
        scratch_shapes=[pltpu.SemaphoreType.DMA],
        compiler_params=pltpu.CompilerParams(vmem_limit_bytes=PACK_VMEM * 1024 * 1024),
        cost_estimate=pl.CostEstimate(
            flops=1_000_000, bytes_accessed=4 * packed.size, transcendentals=0
        ),
        name="pack",
    )(page_table, migration, keys, values)


def place_kernel(lengths, migration, dest_slots, packed, key_area, value_area, blank, ksem, vsem):
    inst = lax.axis_index("inst")
    pages, moves = dest_slots.shape
    half = packed.shape[0] // 2
    blank[...] = jnp.zeros_like(blank)
    for m in range(moves):
        from_inst = 1 if m < moves // 2 else 0
        held = lengths[from_inst, migration[0, m]]
        for p in range(pages):
            target = pl.ds(pl.multiple_of(dest_slots[p, m] * PAGE, PAGE), PAGE)
            at = (m % (moves // 2) * pages + p) * PAGE
            live = (inst != from_inst) & (p * PAGE < held)
            for area, sem, offset in ((key_area, ksem, at), (value_area, vsem, half + at)):

                @pl.when(live)
                def _():
                    pltpu.make_async_copy(
                        packed.at[pl.ds(offset, PAGE)], area.at[target], sem
                    ).start()

                @pl.when(jnp.logical_not(live))
                def _():
                    pltpu.make_async_copy(blank, area.at[target], sem).start()

    for area, sem in ((key_area, ksem), (value_area, vsem)):
        pltpu.make_async_copy(area, area, sem).wait()


def place(lengths, migration, dest_slots, packed):
    area = jax.ShapeDtypeStruct((dest_slots.size * PAGE, packed.shape[1]), packed.dtype)
    return pl.pallas_call(
        place_kernel,
        out_shape=(area, area),
        in_specs=[SMEM, SMEM, SMEM, VMEM],
        out_specs=(HBM, HBM),
        scratch_shapes=[
            pltpu.VMEM((PAGE, packed.shape[1]), packed.dtype),
            pltpu.SemaphoreType.DMA,
            pltpu.SemaphoreType.DMA,
        ],
        compiler_params=pltpu.CompilerParams(vmem_limit_bytes=PACK_VMEM * 1024 * 1024),
        cost_estimate=pl.CostEstimate(
            flops=1_000_000, bytes_accessed=4 * area.size, transcendentals=0
        ),
        name="place",
    )(lengths, migration, dest_slots, packed)


def body(lengths, page_table, migration, dest_slots, queries, key_cache, value_cache, out_weight):
    parts = lax.axis_size("pipe") * lax.axis_size("tensor")
    (lengths, page_table, migration, dest_slots, queries, keys, values, weight) = [
        pltpu.with_memory_space_constraint(array, pltpu.HBM)
        for array in (
            lengths,
            jnp.transpose(page_table, (2, 0, 1)),
            migration.T,
            dest_slots.T,
            queries.reshape(queries.shape[2:]),
            key_cache.reshape(key_cache.shape[3:]),
            value_cache.reshape(value_cache.shape[3:]),
            out_weight.reshape(out_weight.shape[1:]),
        )
    ]
    partial = attend_project(lengths, page_table, queries, keys, values, weight, parts)
    arrived = lax.all_to_all(partial, ("pipe", "tensor"), split_axis=0, concat_axis=0, tiled=True)
    packed = pack(page_table, migration, keys, values)
    moved = lax.ppermute(packed, "inst", [(0, 1), (1, 0)])
    received = place(lengths, migration, dest_slots, moved)
    update = arrived.astype(jnp.float32).sum(axis=0).astype(jnp.bfloat16)
    return (update[None], *[r.reshape(1, 1, 1, *r.shape) for r in received])


def solution(mesh):
    placed = (
        P(),
        P("inst", None, None),
        P(),
        P(),
        P("inst", "pipe", None, "tensor"),
        P("inst", "pipe", "tensor", None, None),
        P("inst", "pipe", "tensor", None, None),
        P("pipe", "tensor", None),
    )
    return jax.shard_map(
        body,
        mesh=mesh,
        in_specs=placed,
        out_specs=(
            P("inst", None, ("pipe", "tensor")),
            P("inst", "pipe", "tensor", None, None),
            P("inst", "pipe", "tensor", None, None),
        ),
        check_vma=False,
    )
```
